32 devices in a mesh: row: 8 (over y, x, core), col: 4 (over z).
Axes of the slice: x: 2, y: 2, z: 4, core: 2. Of those that a mesh axis runs over, the one named last changes fastest.
Arguments:
- pair: bfloat16 [256, 256, 128], P('row', 'col'), may hold values from -6 to 6
- group: bfloat16 [32, 256, 128], P('col', 'row'), may hold values from -6 to 6
- w_query: bfloat16 [128, 128], replicated, may hold values from -0.5 to 0.5
- w_key: bfloat16 [128, 128], replicated, may hold values from -0.5 to 0.5
- w_value: bfloat16 [128, 128], replicated, may hold values from -0.5 to 0.5
- w_gate: bfloat16 [128, 128], replicated, may hold values from -0.5 to 0.5
- w_bias: float32 [128, 4], replicated, may hold values from -40 to 40
- w_out: bfloat16 [128, 128], replicated, may hold values from -0.5 to 0.5
Outputs:
- update: bfloat16 [32, 256, 128], P('col', 'row')
The draws below stay inside these ranges and needn't reach their ends.
All inputs are finite; a program needn't handle non-finite values.
Results may differ from the reference program's by a relative error of at most 0.012.
Values may be sent and summed in bfloat16 or wider, within the bound.
No kernel may reach another device: no remote copies, remote signals or barrier semaphores. Data moves between devices by JAX's collectives and lax.ppermute only.
A program may use at most 64 MiB of HBM per device.

```python
import math
import jax
import jax.numpy as jnp
from jax import lax

C = 128
H = 4
DH = 32
L = 256
Q = 32


def draw_w_bias(key, part):
    base = jax.random.normal(key, (C, H), jnp.float32) / math.sqrt(C)
    return jnp.clip(base, -40.0, 40.0)


def steps_of(stream_key, extent, shards, smallest, top_value):
    def one(position, shards_of):
        heights = jax.random.uniform(jax.random.fold_in(jax.random.fold_in(stream_key, 6), position), (shards_of,), jnp.float32, smallest / len(shards), top_value / len(shards))
        return jnp.repeat(jnp.exp(heights), extent[position] // shards_of).reshape((-1,) + (1,) * (len(extent) - position - 1))

    factor_of = one(*shards[0])
    for cut in shards[1:]:
        factor_of = factor_of * one(*cut)
    return factor_of


def centred(rng, shape, scale, reach, pieces=(), dtype=jnp.bfloat16):
    values = jax.random.normal(rng, shape, jnp.float32) * scale
    if len(pieces) > 0:
        values = steps_of(rng, shape, pieces, -0.22, 0.18) * values
    return jnp.clip(values, min=-reach, max=reach).astype(dtype)


def setup_inputs(seed: int = 0) -> dict:
    streams_of = jax.random.split(jax.random.key(seed), 9)
    pair = centred(streams_of[0], (L, L, C), 1.0, 6.0, ((0, 8), (1, 4)))
    group = centred(streams_of[1], (Q, L, C), 1.0, 6.0, ((0, 4), (1, 8)))
    w_query = centred(streams_of[2], (C, H * DH), C ** -0.5, 0.5)
    w_key = centred(streams_of[3], (C, H * DH), C ** -0.5, 0.5)
    w_value = centred(streams_of[4], (C, H * DH), C ** -0.5, 0.5)
    w_gate = centred(streams_of[5], (C, H * DH), C ** -0.5, 0.5)
    w_bias = draw_w_bias(jax.random.fold_in(streams_of[8], 71), 0)
    w_out = centred(streams_of[7], (H * DH, C), (H * DH) ** -0.5, 0.5)
    return {"pair": pair, "group": group, "w_query": w_query, "w_key": w_key, "w_value": w_value, "w_gate": w_gate, "w_bias": w_bias, "w_out": w_out}


EPS = 1e-05

def normalize(entries):
    average = lax.optimization_barrier(jnp.mean(entries, axis=-1, keepdims=True))
    centered = entries - average
    spread = lax.optimization_barrier(jnp.mean(centered * centered, axis=-1, keepdims=True))
    return centered * lax.rsqrt(spread + EPS)

def reference(pair, group, w_query, w_key, w_value, w_gate, w_bias, w_out):

    def bias_row(pair_row):
        return jnp.dot(normalize(pair_row.astype(jnp.float32)), w_bias, precision=lax.Precision.HIGHEST)
    bias = jnp.transpose(lax.map(bias_row, pair), (2, 0, 1))
    query_count = group.shape[0]
    residues = group.shape[1]
    normed = normalize(group.astype(jnp.float32)).astype(jnp.bfloat16)
    flat_rows = normed.reshape(-1, C)
    scale = 1.0 / math.sqrt(DH)
    query = (jnp.dot(flat_rows, w_query, preferred_element_type=jnp.float32) * scale).astype(jnp.bfloat16)
    key = jnp.dot(flat_rows, w_key, preferred_element_type=jnp.float32).astype(jnp.bfloat16)
    value = jnp.dot(flat_rows, w_value, preferred_element_type=jnp.float32).astype(jnp.bfloat16)
    gating = jax.nn.sigmoid(jnp.dot(flat_rows, w_gate, preferred_element_type=jnp.float32))
    shape4 = (query_count, residues, H, DH)

    def one_row(items):
        query_row, key_row, value_row = items
        scores = jnp.einsum('jhd,khd->hjk', query_row.astype(jnp.float32), key_row.astype(jnp.float32)) + bias
        row_top = lax.optimization_barrier(jnp.max(scores, axis=-1, keepdims=True))
        weights = jnp.exp(scores - row_top)
        row_sum = lax.optimization_barrier(jnp.sum(weights, axis=-1))
        weights_b = weights.astype(jnp.bfloat16).astype(jnp.float32)
        mixture = jnp.einsum('hjk,khd->jhd', weights_b, value_row.astype(jnp.float32))
        return (mixture / jnp.transpose(row_sum)[:, :, None]).reshape(residues, H * DH)
    attention = lax.map(one_row, (query.reshape(shape4), key.reshape(shape4), value.reshape(shape4)))
    hidden = (gating * attention.reshape(-1, H * DH)).astype(jnp.bfloat16)
    result = jnp.dot(hidden, w_out, preferred_element_type=jnp.float32).astype(jnp.bfloat16)
    return result.reshape(query_count, residues, C)
```

```python
import math

import jax
import jax.numpy as jnp
from jax import lax
from jax.experimental import pallas as pl
from jax.experimental.pallas import tpu as pltpu
from jax.sharding import PartitionSpec as P

EPS = 1e-05
NT = (((1,), (1,)), ((), ()))
GRANT = 16 << 20
VMEM = pl.BlockSpec(memory_space=pltpu.VMEM)


def call(kernel, outs, args, flops, scratch=()):
    return pl.pallas_call(
        kernel,
        out_shape=outs,
        in_specs=[VMEM] * len(args),
        out_specs=jax.tree.map(lambda _: VMEM, outs),
        scratch_shapes=list(scratch),
        cost_estimate=pl.CostEstimate(flops=flops, bytes_accessed=1 << 20, transcendentals=0),
        compiler_params=pltpu.CompilerParams(vmem_limit_bytes=GRANT),
    )(*args)


def dot(a, b):
    return jnp.dot(a, b, preferred_element_type=jnp.float32)


def norm_kernel(group_ref, out_ref):
    rows = group_ref[...].astype(jnp.float32)
    centered = rows - jnp.mean(rows, axis=-1, keepdims=True)
    spread = jnp.mean(centered * centered, axis=-1, keepdims=True)
    out_ref[...] = (centered * lax.rsqrt(spread + EPS)).astype(jnp.bfloat16)


def split(value):
    high = value.astype(jnp.bfloat16)
    return high, value - high.astype(jnp.float32)


def bias_kernel(pair_ref, w_ref, out_ref):
    cols, keys, channels = pair_ref.shape
    heads = w_ref.shape[0]
    half = cols // 2
    ones = jnp.full((8, channels), 1.0 / channels, jnp.bfloat16)
    w = jnp.concatenate([w_ref[...]] * (8 // heads), axis=0)
    w_high, rest = split(w)
    w_mid, rest = split(rest)
    w_low = rest.astype(jnp.bfloat16)
    w_sum = jnp.sum(w, axis=1, keepdims=True)
    left = jnp.concatenate([w_high, w_mid, w_low, ones], axis=0)
    square = jnp.full((channels, channels), 1.0 / channels, jnp.bfloat16)
    for low in range(half):
        tile = jnp.concatenate([pair_ref[low], pair_ref[low + half]], axis=0)
        mean = dot(tile, square)
        centered = tile.astype(jnp.float32) - mean
        high, rest = split(centered * centered)
        both = lax.dot_general(left, tile, NT, preferred_element_type=jnp.float32)
        spread = lax.dot_general(
            ones, high, NT, preferred_element_type=jnp.float32
        ) + lax.dot_general(
            ones, rest.astype(jnp.bfloat16), NT, preferred_element_type=jnp.float32
        )
        total = both[0:8] + both[8:16] + both[16:24] - both[24:32] * w_sum
        bias = total * lax.rsqrt(spread + EPS)
        out_ref[pl.ds((low // 8) * 8 * heads + low % 8, heads, stride=8), :] = bias[0:heads]


def scores_kernel(heads, parts, *refs):
    blocks = refs[:parts]
    wq_ref, wk_ref, wv_ref, wg_ref, score_ref, value_ref, gate_ref, key_ref = refs[parts:]
    rows, cols, channels = blocks[0].shape
    width = wq_ref.shape[1]
    depth = width // heads
    me = lax.axis_index("row")
    own = blocks[0][...].reshape(rows * cols, channels)
    both = dot(own, jnp.concatenate([wq_ref[...], wg_ref[...]], axis=1))
    gate_ref[...] = jax.nn.sigmoid(both[:, width:]).reshape(rows, cols, width)
    query = both[:, :width] * (1.0 / math.sqrt(depth))
    w_kv = jnp.concatenate([wk_ref[...], wv_ref[...]], axis=1)
    for step in range(parts):
        block = blocks[step][...].reshape(rows * cols, channels)
        place = pl.ds(pl.multiple_of((me ^ step) * cols, cols), cols)
        kv = dot(block, w_kv).astype(jnp.bfloat16).reshape(rows, cols, 2 * width)
        key_ref[:, place, :] = kv[:, :, :width]
        value_ref[:, place, :] = kv[:, :, width:]
    lane = lax.broadcasted_iota(jnp.int32, (8, width), 1) // depth
    for row in range(rows):
        tiles = []
        for g in range(cols // 8):
            tile = query[row * cols + g * 8 : row * cols + g * 8 + 8]
            for h in range(heads):
                tiles.append(jnp.where(lane == h, tile, 0.0))
        stacked = jnp.concatenate(tiles, axis=0).astype(jnp.bfloat16)
        score_ref[row] = lax.dot_general(
            stacked, key_ref[row], NT, preferred_element_type=jnp.float32
        )


def attention_kernel(heads, parts, *refs):
    panels = refs[:parts]
    score_ref, value_ref, gate_ref, wo_ref, out_ref, bias_ref, hidden_ref = refs[parts:]
    rows, cols, width = gate_ref.shape
    depth = width // heads
    keys = panels[0].shape[1] // 2
    half = panels[0].shape[0]
    me = lax.axis_index("col")
    p = [r[...] for r in panels]
    bit = 1
    while bit < parts:
        flip = (me & bit) != 0
        p = [jnp.where(flip, p[s ^ bit], p[s]) for s in range(parts)]
        bit *= 2
    for h in range(2):
        for c in range(0, parts, 2):
            bias_ref[h * half : (h + 1) * half, c * keys : (c + 2) * keys] = jnp.concatenate(
                [x[:, h * keys : (h + 1) * keys] for x in p[c : c + 2]], axis=1
            )
    lane = lax.broadcasted_iota(jnp.int32, (8, width), 1) // depth
    ones = jnp.ones((value_ref.shape[1], width), jnp.bfloat16)
    for row in range(rows):
        scores = score_ref[row] + bias_ref[...]
        top = jnp.max(scores, axis=1, keepdims=True)
        weights = jnp.exp(scores - top).astype(jnp.bfloat16)
        both = dot(weights, jnp.concatenate([value_ref[row], ones], axis=1))
        for g in range(cols // 8):
            base = g * heads * 8
            pick = both[base : base + 8]
            for h in range(1, heads):
                tile = both[base + h * 8 : base + h * 8 + 8]
                keep = lane == h
                pick = jnp.where(jnp.concatenate([keep, keep], axis=1), tile, pick)
            mixed = pick[:, :width] / pick[:, width:]
            hidden_ref[row * cols + g * 8 : row * cols + g * 8 + 8] = (
                gate_ref[row, g * 8 : g * 8 + 8] * mixed
            )
    result = dot(hidden_ref[...].astype(jnp.bfloat16), wo_ref[...])
    out_ref[...] = result.astype(jnp.bfloat16).reshape(out_ref.shape)


def swap(value, axis, size, distance):
    return lax.ppermute(value, axis, [(i, i ^ distance) for i in range(size)])


def per_device(row_size, col_size, pair, group, w_query, w_key, w_value, w_gate, w_bias, w_out):
    heads = w_bias.shape[1]
    rows, cols, channels = group.shape
    width = w_query.shape[1]
    keys = pair.shape[1]
    all_keys = row_size * cols
    shape = jax.ShapeDtypeStruct
    normed = call(norm_kernel, shape(group.shape, jnp.bfloat16), [group], 10**8)
    blocks = {0: normed}
    for distance in range(2, row_size, 2):
        blocks[distance] = swap(normed, "row", row_size, distance)
    for distance in range(0, row_size, 2):
        blocks[distance + 1] = swap(blocks[distance], "row", row_size, 1)
    panel = call(
        bias_kernel,
        shape((cols * heads // 2, 2 * keys), jnp.float32),
        [pair, w_bias.T],
        2 * 10**9,
    )
    panels = [panel] + [swap(panel, "col", col_size, s) for s in range(1, col_size)]
    scores, value, gate = call(
        lambda *refs: scores_kernel(heads, row_size, *refs),
        (
            shape((rows, cols * heads, all_keys), jnp.float32),
            shape((rows, all_keys, width), jnp.bfloat16),
            shape((rows, cols, width), jnp.float32),
        ),
        [blocks[s] for s in range(row_size)] + [w_query, w_key, w_value, w_gate],
        10**9,
        [pltpu.VMEM((rows, all_keys, width), jnp.bfloat16)],
    )
    return call(
        lambda *refs: attention_kernel(heads, col_size, *refs),
        shape((rows, cols, w_out.shape[1]), jnp.bfloat16),
        panels + [scores, value, gate, w_out],
        10**9,
        [
            pltpu.VMEM((cols * heads, all_keys), jnp.float32),
            pltpu.VMEM((rows * cols, width), jnp.float32),
        ],
    )


def solution(mesh):
    row_size, col_size = mesh.shape["row"], mesh.shape["col"]
    in_specs = (P("row", "col", None), P("col", "row", None), P(), P(), P(), P(), P(), P())
    return jax.shard_map(
        lambda *args: per_device(row_size, col_size, *args),
        mesh=mesh,
        in_specs=in_specs,
        out_specs=P("col", "row", None),
        check_vma=False,
    )
```

```python
import math

import jax
import jax.numpy as jnp
from jax import lax
from jax.experimental import pallas as pl
from jax.experimental.pallas import tpu as pltpu
from jax.sharding import PartitionSpec as P

EPS = 1e-05
NT = (((1,), (1,)), ((), ()))
GRANT = 16 << 20
VMEM = pl.BlockSpec(memory_space=pltpu.VMEM)


def call(kernel, outs, args, flops, scratch=()):
    return pl.pallas_call(
        kernel,
        out_shape=outs,
        in_specs=[VMEM] * len(args),
        out_specs=jax.tree.map(lambda _: VMEM, outs),
        scratch_shapes=list(scratch),
        cost_estimate=pl.CostEstimate(flops=flops, bytes_accessed=1 << 20, transcendentals=0),
        compiler_params=pltpu.CompilerParams(vmem_limit_bytes=GRANT),
    )(*args)


def dot(a, b):
    return jnp.dot(a, b, preferred_element_type=jnp.float32)


def norm_kernel(group_ref, out_ref):
    rows = group_ref[...].astype(jnp.float32)
    centered = rows - jnp.mean(rows, axis=-1, keepdims=True)
    spread = jnp.mean(centered * centered, axis=-1, keepdims=True)
    out_ref[...] = (centered * lax.rsqrt(spread + EPS)).astype(jnp.bfloat16)


def split(value):
    high = value.astype(jnp.bfloat16)
    return high, value - high.astype(jnp.float32)


def bias_kernel(pair_ref, w_ref, out_ref):
    cols, keys, channels = pair_ref.shape
    heads = w_ref.shape[0]
    half = cols // 2
    w = jnp.concatenate([w_ref[...]] * (8 // heads), axis=0)
    w_high, rest = split(w)
    w_mid, rest = split(rest)
    w_sum = jnp.sum(w, axis=1, keepdims=True)
    even = jnp.full((channels, channels), 1.0 / channels, jnp.bfloat16)
    blank = jnp.zeros((channels, channels), jnp.bfloat16)
    averages = jnp.concatenate(
        [jnp.concatenate([even, blank], axis=1), jnp.concatenate([blank, even], axis=1)], axis=0
    )
    pieces = jnp.concatenate([w_high, w_mid, rest.astype(jnp.bfloat16), even[:8]], axis=0)
    left = jnp.concatenate(
        [
            jnp.concatenate([pieces, blank[:96]], axis=0),
            jnp.concatenate([blank[:64], pieces, blank[:32]], axis=0),
        ],
        axis=1,
    )
    tiles = [
        jnp.concatenate([pair_ref[low], pair_ref[low + half]], axis=0) for low in range(half)
    ]
    twins = jnp.concatenate(
        [jnp.concatenate(tiles[low : low + 2], axis=1) for low in range(0, half, 2)], axis=0
    )
    means = dot(twins, averages)
    products = lax.dot_general(twins, left, NT, preferred_element_type=jnp.float32)
    height = 2 * keys
    lane = lax.broadcasted_iota(jnp.int32, (height, 128), 1)
    for low in range(0, half, 2):
        rows = slice(low // 2 * height, low // 2 * height + height)
        centered = twins[rows].astype(jnp.float32) - means[rows]
        squares = centered * centered
        first = jnp.sum(squares[:, :channels], axis=1, keepdims=True)
        second = jnp.sum(squares[:, channels:], axis=1, keepdims=True)
        mixed = jnp.where(
            (lane & 32) == 0, products[rows], jnp.where(lane < 64, first, second)
        ).T
        for twin in range(2):
            t = mixed[twin * 64 : twin * 64 + 64]
            total = t[0:8] + t[8:16] + t[16:24] - t[24:32] * w_sum
            bias = total * lax.rsqrt(t[32:40] * (1.0 / channels) + EPS)
            at = low + twin
            out_ref[pl.ds((at // 8) * 8 * heads + at % 8, heads, stride=8), :] = bias[0:heads]


def scores_kernel(heads, parts, *refs):
    blocks = refs[:parts]
    wq_ref, wk_ref, wv_ref, wg_ref, score_ref, value_ref, gate_ref, key_ref = refs[parts:]
    rows, cols, channels = blocks[0].shape
    width = wq_ref.shape[1]
    depth = width // heads
    me = lax.axis_index("row")
    own = blocks[0][...].reshape(rows * cols, channels)
    both = dot(own, jnp.concatenate([wq_ref[...], wg_ref[...]], axis=1))
    gate_ref[...] = jax.nn.sigmoid(both[:, width:]).reshape(rows, cols, width)
    query = both[:, :width] * (1.0 / math.sqrt(depth))
    w_kv = jnp.concatenate([wk_ref[...], wv_ref[...]], axis=1)
    for step in range(parts):
        block = blocks[step][...].reshape(rows * cols, channels)
        place = pl.ds(pl.multiple_of((me ^ step) * cols, cols), cols)
        kv = dot(block, w_kv).astype(jnp.bfloat16).reshape(rows, cols, 2 * width)
        key_ref[:, place, :] = kv[:, :, :width]
        value_ref[:, place, :] = kv[:, :, width:]
    lane = lax.broadcasted_iota(jnp.int32, (8, width), 1) // depth
    for row in range(rows):
        tiles = []
        for g in range(cols // 8):
            tile = query[row * cols + g * 8 : row * cols + g * 8 + 8]
            for h in range(heads):
                tiles.append(jnp.where(lane == h, tile, 0.0))
        stacked = jnp.concatenate(tiles, axis=0).astype(jnp.bfloat16)
        score_ref[row] = lax.dot_general(
            stacked, key_ref[row], NT, preferred_element_type=jnp.float32
        )


def attention_kernel(heads, parts, *refs):
    panels = refs[:parts]
    score_ref, value_ref, gate_ref, wo_ref, out_ref, bias_ref, hidden_ref = refs[parts:]
    rows, cols, width = gate_ref.shape
    depth = width // heads
    keys = panels[0].shape[1] // 2
    half = panels[0].shape[0]
    me = lax.axis_index("col")
    p = [r[...] for r in panels]
    bit = 1
    while bit < parts:
        flip = (me & bit) != 0
        p = [jnp.where(flip, p[s ^ bit], p[s]) for s in range(parts)]
        bit *= 2
    for h in range(2):
        for c in range(0, parts, 2):
            bias_ref[h * half : (h + 1) * half, c * keys : (c + 2) * keys] = jnp.concatenate(
                [x[:, h * keys : (h + 1) * keys] for x in p[c : c + 2]], axis=1
            )
    lane = lax.broadcasted_iota(jnp.int32, (8, width), 1) // depth
    ones = jnp.ones((value_ref.shape[1], width), jnp.bfloat16)
    for row in range(rows):
        scores = score_ref[row] + bias_ref[...]
        top = jnp.max(scores, axis=1, keepdims=True)
        weights = jnp.exp(scores - top).astype(jnp.bfloat16)
        both = dot(weights, jnp.concatenate([value_ref[row], ones], axis=1))
        for g in range(cols // 8):
            base = g * heads * 8
            pick = both[base : base + 8]
            for h in range(1, heads):
                tile = both[base + h * 8 : base + h * 8 + 8]
                keep = lane == h
                pick = jnp.where(jnp.concatenate([keep, keep], axis=1), tile, pick)
            mixed = pick[:, :width] / pick[:, width:]
            hidden_ref[row * cols + g * 8 : row * cols + g * 8 + 8] = (
                gate_ref[row, g * 8 : g * 8 + 8] * mixed
            )
    result = dot(hidden_ref[...].astype(jnp.bfloat16), wo_ref[...])
    out_ref[...] = result.astype(jnp.bfloat16).reshape(out_ref.shape)


def swap(value, axis, size, distance):
    return lax.ppermute(value, axis, [(i, i ^ distance) for i in range(size)])


def per_device(row_size, col_size, pair, group, w_query, w_key, w_value, w_gate, w_bias, w_out):
    heads = w_bias.shape[1]
    rows, cols, channels = group.shape
    width = w_query.shape[1]
    keys = pair.shape[1]
    all_keys = row_size * cols
    shape = jax.ShapeDtypeStruct
    normed = call(norm_kernel, shape(group.shape, jnp.bfloat16), [group], 10**8)
    blocks = {0: normed}
    for distance in range(2, row_size, 2):
        blocks[distance] = swap(normed, "row", row_size, distance)
    for distance in range(0, row_size, 2):
        blocks[distance + 1] = swap(blocks[distance], "row", row_size, 1)
    panel = call(
        bias_kernel,
        shape((cols * heads // 2, 2 * keys), jnp.float32),
        [pair, w_bias.T],
        2 * 10**9,
    )
    panels = [panel] + [swap(panel, "col", col_size, s) for s in range(1, col_size)]
    scores, value, gate = call(
        lambda *refs: scores_kernel(heads, row_size, *refs),
        (
            shape((rows, cols * heads, all_keys), jnp.float32),
            shape((rows, all_keys, width), jnp.bfloat16),
            shape((rows, cols, width), jnp.float32),
        ),
        [blocks[s] for s in range(row_size)] + [w_query, w_key, w_value, w_gate],
        10**9,
        [pltpu.VMEM((rows, all_keys, width), jnp.bfloat16)],
    )
    return call(
        lambda *refs: attention_kernel(heads, col_size, *refs),
        shape((rows, cols, w_out.shape[1]), jnp.bfloat16),
        panels + [scores, value, gate, w_out],
        10**9,
        [
            pltpu.VMEM((cols * heads, all_keys), jnp.float32),
            pltpu.VMEM((rows * cols, width), jnp.float32),
        ],
    )


def solution(mesh):
    row_size, col_size = mesh.shape["row"], mesh.shape["col"]
    in_specs = (P("row", "col", None), P("col", "row", None), P(), P(), P(), P(), P(), P())
    return jax.shard_map(
        lambda *args: per_device(row_size, col_size, *args),
        mesh=mesh,
        in_specs=in_specs,
        out_specs=P("col", "row", None),
        check_vma=False,
    )
```

```python
import math

import jax
import jax.numpy as jnp
from jax import lax
from jax.experimental import pallas as pl
from jax.experimental.pallas import tpu as pltpu
from jax.sharding import PartitionSpec as P


EPS = 1e-05
NT = (((1,), (1,)), ((), ()))
GRANT = 16 << 20
VMEM = pl.BlockSpec(memory_space=pltpu.VMEM)


def call(kernel, outs, args, flops, scratch=(), space=pltpu.VMEM):
    return pl.pallas_call(
        kernel,
        out_shape=outs,
        in_specs=[pl.BlockSpec(memory_space=space)] * len(args),
        out_specs=jax.tree.map(lambda _: VMEM, outs),
        scratch_shapes=list(scratch),
        cost_estimate=pl.CostEstimate(flops=flops, bytes_accessed=1 << 20, transcendentals=0),
        compiler_params=pltpu.CompilerParams(vmem_limit_bytes=GRANT),
    )(*args)


def dot(a, b):
    return jnp.dot(a, b, preferred_element_type=jnp.float32)


def split(value):
    high = value.astype(jnp.bfloat16)
    return high, value - high.astype(jnp.float32)


def front_kernel(*refs):
    sources, (normed_ref, out_ref), landed, semaphores = refs[:3], refs[3:5], refs[5:8], refs[8]
    copies = [
        pltpu.make_async_copy(a, b, semaphores.at[i])
        for i, (a, b) in enumerate(zip(sources, landed))
    ]
    for copy in copies:
        copy.start()
    group_ref, pair_ref, w_ref = landed
    copies[0].wait()
    rows = group_ref[...].astype(jnp.float32)
    centered = rows - jnp.mean(rows, axis=-1, keepdims=True)
    spread = jnp.mean(centered * centered, axis=-1, keepdims=True)
    normed_ref[...] = (centered * lax.rsqrt(spread + EPS)).astype(jnp.bfloat16)
    copies[1].wait()
    copies[2].wait()
    cols, keys, channels = pair_ref.shape
    heads = w_ref.shape[0]
    half = cols // 2
    w = jnp.concatenate([w_ref[...]] * (8 // heads), axis=0)
    w_high, rest = split(w)
    w_mid, rest = split(rest)
    w_sum = jnp.sum(w, axis=1, keepdims=True)
    even = jnp.full((channels, channels), 1.0 / channels, jnp.bfloat16)
    blank = jnp.zeros((channels, channels), jnp.bfloat16)
    averages = jnp.concatenate(
        [jnp.concatenate([even, blank], axis=1), jnp.concatenate([blank, even], axis=1)], axis=0
    )
    pieces = jnp.concatenate([w_high, w_mid, rest.astype(jnp.bfloat16), even[:8]], axis=0)
    left = jnp.concatenate(
        [
            jnp.concatenate([pieces, blank[:96]], axis=0),
            jnp.concatenate([blank[:64], pieces, blank[:32]], axis=0),
        ],
        axis=1,
    )
    tiles = [
        jnp.concatenate([pair_ref[low], pair_ref[low + half]], axis=0) for low in range(half)
    ]
    twins = jnp.concatenate(
        [jnp.concatenate(tiles[low : low + 2], axis=1) for low in range(0, half, 2)], axis=0
    )
    means = dot(twins, averages)
    products = lax.dot_general(twins, left, NT, preferred_element_type=jnp.float32)
    height = 2 * keys
    lane = lax.broadcasted_iota(jnp.int32, (height, 128), 1)
    for low in range(0, half, 2):
        rows = slice(low // 2 * height, low // 2 * height + height)
        centered = twins[rows].astype(jnp.float32) - means[rows]
        squares = centered * centered
        first = jnp.sum(squares[:, :channels], axis=1, keepdims=True)
        second = jnp.sum(squares[:, channels:], axis=1, keepdims=True)
        mixed = jnp.where(
            (lane & 32) == 0, products[rows], jnp.where(lane < 64, first, second)
        ).T
        for twin in range(2):
            t = mixed[twin * 64 : twin * 64 + 64]
            total = t[0:8] + t[8:16] + t[16:24] - t[24:32] * w_sum
            bias = total * lax.rsqrt(t[32:40] * (1.0 / channels) + EPS)
            at = low + twin
            out_ref[pl.ds((at // 8) * 8 * heads + at % 8, heads, stride=8), :] = bias[0:heads]


def scores_kernel(heads, parts, *refs):
    blocks = refs[:parts]
    wq_ref, wk_ref, wv_ref, wg_ref, score_ref, value_ref, gate_ref, key_ref = refs[parts:]
    rows, cols, channels = blocks[0].shape
    width = wq_ref.shape[1]
    depth = width // heads
    me = lax.axis_index("row")
    own = blocks[0][...].reshape(rows * cols, channels)
    both = dot(own, jnp.concatenate([wq_ref[...], wg_ref[...]], axis=1))
    gate_ref[...] = jax.nn.sigmoid(both[:, width:]).reshape(rows, cols, width)
    query = both[:, :width] * (1.0 / math.sqrt(depth))
    w_kv = jnp.concatenate([wk_ref[...], wv_ref[...]], axis=1)
    for step in range(parts):
        block = blocks[step][...].reshape(rows * cols, channels)
        place = pl.ds(pl.multiple_of((me ^ step) * cols, cols), cols)
        kv = dot(block, w_kv).astype(jnp.bfloat16).reshape(rows, cols, 2 * width)
        key_ref[:, place, :] = kv[:, :, :width]
        value_ref[:, place, :] = kv[:, :, width:]
    lane = lax.broadcasted_iota(jnp.int32, (8, width), 1) // depth
    for row in range(rows):
        tiles = []
        for g in range(cols // 8):
            tile = query[row * cols + g * 8 : row * cols + g * 8 + 8]
            for h in range(heads):
                tiles.append(jnp.where(lane == h, tile, 0.0))
        stacked = jnp.concatenate(tiles, axis=0).astype(jnp.bfloat16)
        score_ref[row] = lax.dot_general(
            stacked, key_ref[row], NT, preferred_element_type=jnp.float32
        )


def attention_kernel(heads, parts, *refs):
    panels = refs[:parts]
    score_ref, value_ref, gate_ref, wo_ref, out_ref, bias_ref, hidden_ref = refs[parts:]
    rows, cols, width = gate_ref.shape
    depth = width // heads
    keys = panels[0].shape[1] // 2
    half = panels[0].shape[0]
    me = lax.axis_index("col")
    p = [r[...] for r in panels]
    bit = 1
    while bit < parts:
        flip = (me & bit) != 0
        p = [jnp.where(flip, p[s ^ bit], p[s]) for s in range(parts)]
        bit *= 2
    for h in range(2):
        for c in range(0, parts, 2):
            bias_ref[h * half : (h + 1) * half, c * keys : (c + 2) * keys] = jnp.concatenate(
                [x[:, h * keys : (h + 1) * keys] for x in p[c : c + 2]], axis=1
            )
    lane = lax.broadcasted_iota(jnp.int32, (8, width), 1) // depth
    ones = jnp.ones((value_ref.shape[1], width), jnp.bfloat16)
    for row in range(rows):
        scores = score_ref[row] + bias_ref[...]
        top = jnp.max(scores, axis=1, keepdims=True)
        weights = jnp.exp(scores - top).astype(jnp.bfloat16)
        both = dot(weights, jnp.concatenate([value_ref[row], ones], axis=1))
        for g in range(cols // 8):
            base = g * heads * 8
            pick = both[base : base + 8]
            for h in range(1, heads):
                tile = both[base + h * 8 : base + h * 8 + 8]
                keep = lane == h
                pick = jnp.where(jnp.concatenate([keep, keep], axis=1), tile, pick)
            mixed = pick[:, :width] / pick[:, width:]
            hidden_ref[row * cols + g * 8 : row * cols + g * 8 + 8] = (
                gate_ref[row, g * 8 : g * 8 + 8] * mixed
            )
    result = dot(hidden_ref[...].astype(jnp.bfloat16), wo_ref[...])
    out_ref[...] = result.astype(jnp.bfloat16).reshape(out_ref.shape)


def swap(value, axis, size, distance):
    return lax.ppermute(value, axis, [(i, i ^ distance) for i in range(size)])


def per_device(row_size, col_size, pair, group, w_query, w_key, w_value, w_gate, w_bias, w_out):
    heads = w_bias.shape[1]
    rows, cols, _ = group.shape
    width = w_query.shape[1]
    keys = pair.shape[1]
    all_keys = row_size * cols
    shape = jax.ShapeDtypeStruct
    normed, panel = call(
        front_kernel,
        (
            shape(group.shape, jnp.bfloat16),
            shape((cols * heads // 2, 2 * keys), jnp.float32),
        ),
        [pltpu.with_memory_space_constraint(a, pltpu.HBM) for a in (group, pair, w_bias.T)],
        2 * 10**9,
        [pltpu.VMEM(a.shape, a.dtype) for a in (group, pair, w_bias.T)]
        + [pltpu.SemaphoreType.DMA((3,))],
        pltpu.HBM,
    )
    blocks = {0: normed}
    for s in range(2, row_size, 2):
        blocks[s] = swap(normed, "row", row_size, s)
    for s in range(0, row_size, 2):
        blocks[s + 1] = swap(blocks[s], "row", row_size, 1)
    panels = [panel] + [swap(panel, "col", col_size, s) for s in range(1, col_size)]
    scores, value, gate = call(
        lambda *refs: scores_kernel(heads, row_size, *refs),
        (
            shape((rows, cols * heads, all_keys), jnp.float32),
            shape((rows, all_keys, width), jnp.bfloat16),
            shape((rows, cols, width), jnp.float32),
        ),
        [blocks[s] for s in range(row_size)] + [w_query, w_key, w_value, w_gate],
        10**9,
        [pltpu.VMEM((rows, all_keys, width), jnp.bfloat16)],
    )
    return call(
        lambda *refs: attention_kernel(heads, col_size, *refs),
        shape((rows, cols, w_out.shape[1]), jnp.bfloat16),
        panels + [scores, value, gate, w_out],
        10**9,
        [
            pltpu.VMEM((cols * heads, all_keys), jnp.float32),
            pltpu.VMEM((rows * cols, width), jnp.float32),
        ],
    )


def solution(mesh):
    row_size, col_size = mesh.shape["row"], mesh.shape["col"]
    in_specs = (P("row", "col", None), P("col", "row", None), P(), P(), P(), P(), P(), P())

    def body(*args):
        return per_device(row_size, col_size, *args)

    return jax.shard_map(
        body,
        mesh=mesh,
        in_specs=in_specs,
        out_specs=P("col", "row", None),
        check_vma=False,
    )
```

```python
import math

import jax
import jax.numpy as jnp
from jax import lax
from jax.experimental import pallas as pl
from jax.experimental.pallas import tpu as pltpu
from jax.sharding import PartitionSpec as P


EPS = 1e-05
NT = (((1,), (1,)), ((), ()))
GRANT = 16 << 20
VMEM = pl.BlockSpec(memory_space=pltpu.VMEM)


def call(kernel, outs, args, flops, scratch=(), space=pltpu.VMEM):
    return pl.pallas_call(
        kernel,
        out_shape=outs,
        in_specs=[pl.BlockSpec(memory_space=space)] * len(args),
        out_specs=jax.tree.map(lambda _: VMEM, outs),
        scratch_shapes=list(scratch),
        cost_estimate=pl.CostEstimate(flops=flops, bytes_accessed=1 << 20, transcendentals=0),
        compiler_params=pltpu.CompilerParams(vmem_limit_bytes=GRANT),
    )(*args)


def dot(a, b):
    return jnp.dot(a, b, preferred_element_type=jnp.float32)


def split(value):
    high = value.astype(jnp.bfloat16)
    return high, value - high.astype(jnp.float32)


def front_kernel(*refs):
    sources, (normed_ref, out_ref), landed, semaphores = refs[:3], refs[3:5], refs[5:8], refs[8]
    copies = [
        pltpu.make_async_copy(a, b, semaphores.at[i])
        for i, (a, b) in enumerate(zip(sources, landed))
    ]
    for copy in copies:
        copy.start()
    group_ref, pair_ref, w_ref = landed
    copies[0].wait()
    rows = group_ref[...].astype(jnp.float32)
    centered = rows - jnp.mean(rows, axis=-1, keepdims=True)
    spread = jnp.mean(centered * centered, axis=-1, keepdims=True)
    normed_ref[...] = (centered * lax.rsqrt(spread + EPS)).astype(jnp.bfloat16)
    copies[1].wait()
    copies[2].wait()
    cols, keys, channels = pair_ref.shape
    heads = w_ref.shape[0]
    half = cols // 2
    w = jnp.concatenate([w_ref[...]] * (8 // heads), axis=0)
    w_high, rest = split(w)
    w_mid, rest = split(rest)
    w_sum = jnp.sum(w, axis=1, keepdims=True)
    even = jnp.full((channels, channels), 1.0 / channels, jnp.bfloat16)
    blank = jnp.zeros((channels, channels), jnp.bfloat16)
    averages = jnp.concatenate(
        [jnp.concatenate([even, blank], axis=1), jnp.concatenate([blank, even], axis=1)], axis=0
    )
    pieces = jnp.concatenate([w_high, w_mid, rest.astype(jnp.bfloat16), even[:8]], axis=0)
    left = jnp.concatenate(
        [
            jnp.concatenate([pieces, blank[:96]], axis=0),
            jnp.concatenate([blank[:64], pieces, blank[:32]], axis=0),
        ],
        axis=1,
    )
    tiles = [
        jnp.concatenate([pair_ref[low], pair_ref[low + half]], axis=0) for low in range(half)
    ]
    twins = jnp.concatenate(
        [jnp.concatenate(tiles[low : low + 2], axis=1) for low in range(0, half, 2)], axis=0
    )
    means = dot(twins, averages)
    products = lax.dot_general(twins, left, NT, preferred_element_type=jnp.float32)
    height = 2 * keys
    lane = lax.broadcasted_iota(jnp.int32, (height, 128), 1)
    for low in range(0, half, 2):
        rows = slice(low // 2 * height, low // 2 * height + height)
        centered = twins[rows].astype(jnp.float32) - means[rows]
        squares = centered * centered
        first = jnp.sum(squares[:, :channels], axis=1, keepdims=True)
        second = jnp.sum(squares[:, channels:], axis=1, keepdims=True)
        mixed = jnp.where(
            (lane & 32) == 0, products[rows], jnp.where(lane < 64, first, second)
        ).T
        for twin in range(2):
            t = mixed[twin * 64 : twin * 64 + 64]
            total = t[0:8] + t[8:16] + t[16:24] - t[24:32] * w_sum
            bias = total * lax.rsqrt(t[32:40] * (1.0 / channels) + EPS)
            at = low + twin
            out_ref[pl.ds((at // 8) * 8 * heads + at % 8, heads, stride=8), :] = bias[0:heads]


def scores_kernel(heads, origins, *refs):
    sources = len(origins)
    wq_ref, wk_ref, wv_ref, wg_ref, score_ref, value_ref, gate_ref, key_ref = refs[sources:]
    _, rows, cols, channels = refs[0].shape
    width = wq_ref.shape[1]
    depth = width // heads
    me = lax.axis_index("row")
    chips = key_ref.shape[1] // (2 * cols)
    own = refs[0][0].reshape(rows * cols, channels)
    both = dot(own, jnp.concatenate([wq_ref[...], wg_ref[...]], axis=1))
    gate_ref[...] = jax.nn.sigmoid(both[:, width:]).reshape(rows, cols, width)
    query = both[:, :width] * (1.0 / math.sqrt(depth))
    w_kv = jnp.concatenate([wk_ref[...], wv_ref[...]], axis=1)
    for ref, entry, (flip, odd, even) in [
        (ref, entry, origin)
        for ref, group in zip(refs, origins)
        for entry, origin in enumerate(group)
    ]:
        block = ref[entry].reshape(rows * cols, channels)
        core = me & 1
        chip = lax.rem((me >> 1) + chips - jnp.where(core == 1, odd, even), chips)
        place = pl.ds(pl.multiple_of((2 * chip + (core ^ flip)) * cols, cols), cols)
        kv = dot(block, w_kv).astype(jnp.bfloat16).reshape(rows, cols, 2 * width)
        key_ref[:, place, :] = kv[:, :, :width]
        value_ref[:, place, :] = kv[:, :, width:]
    lane = lax.broadcasted_iota(jnp.int32, (8, width), 1) // depth
    for row in range(rows):
        tiles = []
        for g in range(cols // 8):
            tile = query[row * cols + g * 8 : row * cols + g * 8 + 8]
            for h in range(heads):
                tiles.append(jnp.where(lane == h, tile, 0.0))
        stacked = jnp.concatenate(tiles, axis=0).astype(jnp.bfloat16)
        score_ref[row] = lax.dot_general(
            stacked, key_ref[row], NT, preferred_element_type=jnp.float32
        )


def attention_kernel(heads, parts, *refs):
    panels = refs[:parts]
    score_ref, value_ref, gate_ref, wo_ref, out_ref, bias_ref, hidden_ref = refs[parts:]
    rows, cols, width = gate_ref.shape
    depth = width // heads
    keys = panels[0].shape[1] // 2
    half = panels[0].shape[0]
    me = lax.axis_index("col")
    p = [panels[(parts - k) % parts][...] for k in range(parts)]
    bit = 1
    while bit < parts:
        turn = (me & bit) != 0
        p = [jnp.where(turn, p[(k - bit) % parts], p[k]) for k in range(parts)]
        bit *= 2
    for h in range(2):
        for c in range(0, parts, 2):
            bias_ref[h * half : (h + 1) * half, c * keys : (c + 2) * keys] = jnp.concatenate(
                [x[:, h * keys : (h + 1) * keys] for x in p[c : c + 2]], axis=1
            )
    lane = lax.broadcasted_iota(jnp.int32, (8, width), 1) // depth
    ones = jnp.ones((value_ref.shape[1], width), jnp.bfloat16)
    for row in range(rows):
        scores = score_ref[row] + bias_ref[...]
        top = jnp.max(scores, axis=1, keepdims=True)
        weights = jnp.exp(scores - top).astype(jnp.bfloat16)
        both = dot(weights, jnp.concatenate([value_ref[row], ones], axis=1))
        for g in range(cols // 8):
            base = g * heads * 8
            pick = both[base : base + 8]
            for h in range(1, heads):
                tile = both[base + h * 8 : base + h * 8 + 8]
                keep = lane == h
                pick = jnp.where(jnp.concatenate([keep, keep], axis=1), tile, pick)
            mixed = pick[:, :width] / pick[:, width:]
            hidden_ref[row * cols + g * 8 : row * cols + g * 8 + 8] = (
                gate_ref[row, g * 8 : g * 8 + 8] * mixed
            )
    result = dot(hidden_ref[...].astype(jnp.bfloat16), wo_ref[...])
    out_ref[...] = result.astype(jnp.bfloat16).reshape(out_ref.shape)


def swap(value, size):
    return lax.ppermute(value, "row", [(i, i ^ 1) for i in range(size)])


def chip_shift(value, size, odd, even):
    pairs = [(i, (i + 2 * (odd if i % 2 else even)) % size) for i in range(size)]
    return lax.ppermute(value, "row", pairs)


def shift(value, axis, size, distance):
    pairs = [(i, (i + distance) % size) for i in range(size)]
    return lax.ppermute(value, axis, pairs)


def row_plan(row_size):
    shifts = list(reversed(range(1, row_size // 2)))
    single = shifts[: len(shifts) % 2]
    rest = shifts[len(single) :]
    return single, [(rest[i], rest[i + 1]) for i in range(0, len(rest), 2)]


def per_device(row_size, col_size, pair, group, w_query, w_key, w_value, w_gate, w_bias, w_out):
    heads = w_bias.shape[1]
    rows, cols, _ = group.shape
    width = w_query.shape[1]
    keys = pair.shape[1]
    all_keys = row_size * cols
    shape = jax.ShapeDtypeStruct
    normed, panel = call(
        front_kernel,
        (
            shape(group.shape, jnp.bfloat16),
            shape((cols * heads // 2, 2 * keys), jnp.float32),
        ),
        [pltpu.with_memory_space_constraint(a, pltpu.HBM) for a in (group, pair, w_bias.T)],
        2 * 10**9,
        [pltpu.VMEM(a.shape, a.dtype) for a in (group, pair, w_bias.T)]
        + [pltpu.SemaphoreType.DMA((3,))],
        pltpu.HBM,
    )
    normed = normed[None]
    sibling = swap(normed, row_size)
    stacks, origins = [normed, sibling], [[(0, 0, 0)], [(1, 0, 0)]]
    single, plan = row_plan(row_size)
    for s in single:
        arrived = chip_shift(normed, row_size, s, s)
        stacks += [arrived, swap(arrived, row_size)]
        origins += [[(0, s, s)], [(1, s, s)]]
    both = jnp.concatenate([normed, sibling], axis=0)
    for s, t in plan:
        arrived = chip_shift(both, row_size, s, t)
        stacks += [arrived, swap(arrived, row_size)]
        origins += [[(0, s, t), (1, s, t)], [(1, t, s), (0, t, s)]]
    panels = [panel] + [shift(panel, "col", col_size, s) for s in range(1, col_size)]
    scores, value, gate = call(
        lambda *refs: scores_kernel(heads, origins, *refs),
        (
            shape((rows, cols * heads, all_keys), jnp.float32),
            shape((rows, all_keys, width), jnp.bfloat16),
            shape((rows, cols, width), jnp.float32),
        ),
        stacks + [w_query, w_key, w_value, w_gate],
        10**9,
        [pltpu.VMEM((rows, all_keys, width), jnp.bfloat16)],
    )
    return call(
        lambda *refs: attention_kernel(heads, col_size, *refs),
        shape((rows, cols, w_out.shape[1]), jnp.bfloat16),
        panels + [scores, value, gate, w_out],
        10**9,
        [
            pltpu.VMEM((cols * heads, all_keys), jnp.float32),
            pltpu.VMEM((rows * cols, width), jnp.float32),
        ],
    )


def solution(mesh):
    row_size, col_size = mesh.shape["row"], mesh.shape["col"]
    in_specs = (P("row", "col", None), P("col", "row", None), P(), P(), P(), P(), P(), P())

    def body(*args):
        return per_device(row_size, col_size, *args)

    return jax.shard_map(
        body,
        mesh=mesh,
        in_specs=in_specs,
        out_specs=P("col", "row", None),
        check_vma=False,
    )
```

```python
import math

import jax
import jax.numpy as jnp
from jax import lax
from jax.experimental import pallas as pl
from jax.experimental.pallas import tpu as pltpu
from jax.sharding import PartitionSpec as P


EPS = 1e-05
NT = (((1,), (1,)), ((), ()))
GRANT = 16 << 20
VMEM = pl.BlockSpec(memory_space=pltpu.VMEM)


def call(kernel, outs, args, flops, scratch=(), space=pltpu.VMEM, aliases=None):
    return pl.pallas_call(
        kernel,
        out_shape=outs,
        in_specs=[pl.BlockSpec(memory_space=space)] * len(args),
        out_specs=jax.tree.map(lambda _: VMEM, outs),
        scratch_shapes=list(scratch),
        input_output_aliases=aliases or {},
        cost_estimate=pl.CostEstimate(flops=flops, bytes_accessed=1 << 20, transcendentals=0),
        compiler_params=pltpu.CompilerParams(vmem_limit_bytes=GRANT),
    )(*args)


def dot(a, b):
    return jnp.dot(a, b, preferred_element_type=jnp.float32)


def split(value):
    high = value.astype(jnp.bfloat16)
    return high, value - high.astype(jnp.float32)


def load_kernel(group_ref, pair_ref, w_ref, normed_ref, pair_out, w_out, landed, semaphores):
    copies = [
        pltpu.make_async_copy(a, b, semaphores.at[i])
        for i, (a, b) in enumerate(
            [(group_ref, landed), (pair_ref, pair_out), (w_ref, w_out)]
        )
    ]
    for copy in copies:
        copy.start()
    copies[0].wait()
    rows = landed[...].astype(jnp.float32)
    centered = rows - jnp.mean(rows, axis=-1, keepdims=True)
    spread = jnp.mean(centered * centered, axis=-1, keepdims=True)
    normed_ref[...] = (centered * lax.rsqrt(spread + EPS)).astype(jnp.bfloat16)
    copies[1].wait()
    copies[2].wait()


def bias_kernel(pair_ref, w_ref, out_ref):
    cols, keys, channels = pair_ref.shape
    heads = w_ref.shape[0]
    half = cols // 2
    w = jnp.concatenate([w_ref[...]] * (8 // heads), axis=0)
    w_high, rest = split(w)
    w_mid, rest = split(rest)
    w_sum = jnp.sum(w, axis=1, keepdims=True)
    even = jnp.full((channels, channels), 1.0 / channels, jnp.bfloat16)
    blank = jnp.zeros((channels, channels), jnp.bfloat16)
    averages = jnp.concatenate(
        [jnp.concatenate([even, blank], axis=1), jnp.concatenate([blank, even], axis=1)], axis=0
    )
    pieces = jnp.concatenate([w_high, w_mid, rest.astype(jnp.bfloat16), even[:8]], axis=0)
    left = jnp.concatenate(
        [
            jnp.concatenate([pieces, blank[:96]], axis=0),
            jnp.concatenate([blank[:64], pieces, blank[:32]], axis=0),
        ],
        axis=1,
    )
    tiles = [
        jnp.concatenate([pair_ref[low], pair_ref[low + half]], axis=0) for low in range(half)
    ]
    twins = jnp.concatenate(
        [jnp.concatenate(tiles[low : low + 2], axis=1) for low in range(0, half, 2)], axis=0
    )
    means = dot(twins, averages)
    products = lax.dot_general(twins, left, NT, preferred_element_type=jnp.float32)
    height = 2 * keys
    lane = lax.broadcasted_iota(jnp.int32, (height, 128), 1)
    for low in range(0, half, 2):
        rows = slice(low // 2 * height, low // 2 * height + height)
        centered = twins[rows].astype(jnp.float32) - means[rows]
        squares = centered * centered
        first = jnp.sum(squares[:, :channels], axis=1, keepdims=True)
        second = jnp.sum(squares[:, channels:], axis=1, keepdims=True)
        mixed = jnp.where(
            (lane & 32) == 0, products[rows], jnp.where(lane < 64, first, second)
        ).T
        for twin in range(2):
            t = mixed[twin * 64 : twin * 64 + 64]
            total = t[0:8] + t[8:16] + t[16:24] - t[24:32] * w_sum
            bias = total * lax.rsqrt(t[32:40] * (1.0 / channels) + EPS)
            at = low + twin
            out_ref[pl.ds((at // 8) * 8 * heads + at % 8, heads, stride=8), :] = bias[0:heads]


def place_blocks(sources, origins, w_kv, key_ref, value_ref):
    _, rows, cols, channels = sources[0].shape
    width = value_ref.shape[2]
    me = lax.axis_index("row")
    for ref, entry, (flip, odd, even) in [
        (ref, entry, origin)
        for ref, group in zip(sources, origins)
        for entry, origin in enumerate(group)
    ]:
        block = ref[entry].reshape(rows * cols, channels)
        core = me & 1
        chip = (me >> 1) ^ jnp.where(core == 1, odd, even)
        place = pl.ds(pl.multiple_of((2 * chip + (core ^ flip)) * cols, cols), cols)
        kv = dot(block, w_kv).astype(jnp.bfloat16).reshape(rows, cols, 2 * width)
        key_ref[:, place, :] = kv[:, :, :width]
        value_ref[:, place, :] = kv[:, :, width:]


def early_kernel(heads, origins, *refs):
    sources = refs[: len(origins)]
    wq_ref, wk_ref, wv_ref, wg_ref, key_ref, value_ref, gate_ref, stack_ref = refs[len(origins) :]
    _, rows, cols, channels = sources[0].shape
    width = wq_ref.shape[1]
    depth = width // heads
    own = sources[0][0].reshape(rows * cols, channels)
    both = dot(own, jnp.concatenate([wq_ref[...], wg_ref[...]], axis=1))
    gate_ref[...] = jax.nn.sigmoid(both[:, width:]).reshape(rows, cols, width)
    query = both[:, :width] * (1.0 / math.sqrt(depth))
    lane = lax.broadcasted_iota(jnp.int32, (8, width), 1) // depth
    for row in range(rows):
        tiles = []
        for g in range(cols // 8):
            tile = query[row * cols + g * 8 : row * cols + g * 8 + 8]
            for h in range(heads):
                tiles.append(jnp.where(lane == h, tile, 0.0))
        stack_ref[row] = jnp.concatenate(tiles, axis=0).astype(jnp.bfloat16)
    w_kv = jnp.concatenate([wk_ref[...], wv_ref[...]], axis=1)
    place_blocks(sources, origins, w_kv, key_ref, value_ref)


def scores_kernel(origins, *refs):
    sources = refs[: len(origins)]
    stack_ref, wk_ref, wv_ref, _, _, score_ref, key_ref, value_ref = refs[len(origins) :]
    w_kv = jnp.concatenate([wk_ref[...], wv_ref[...]], axis=1)
    place_blocks(sources, origins, w_kv, key_ref, value_ref)
    for row in range(stack_ref.shape[0]):
        score_ref[row] = lax.dot_general(
            stack_ref[row], key_ref[row], NT, preferred_element_type=jnp.float32
        )


def attention_kernel(heads, single, plan, *refs):
    sources = 1 + len(single) + 2 * len(plan)
    score_ref, value_ref, gate_ref, wo_ref, out_ref, bias_ref, hidden_ref = refs[sources:]
    rows, cols, width = gate_ref.shape
    depth = width // heads
    half, keys = refs[0].shape[0], refs[0].shape[1] // 2
    odd = (lax.axis_index("row") & 1) == 1
    me = lax.axis_index("col")
    parts = sources
    p = [refs[0][...]] + [None] * (parts - 1)
    for at, s in enumerate(single):
        p[s] = refs[1 + at][...]
    for at, (s, t) in enumerate(plan):
        arrived = refs[1 + len(single) + 2 * at][:half]
        passed = refs[2 + len(single) + 2 * at][half:]
        p[s] = jnp.where(odd, arrived, passed)
        p[t] = jnp.where(odd, passed, arrived)
    bit = 1
    while bit < parts:
        turn = (me & bit) != 0
        p = [jnp.where(turn, p[k ^ bit], p[k]) for k in range(parts)]
        bit *= 2
    for h in range(2):
        for c in range(0, parts, 2):
            bias_ref[h * half : (h + 1) * half, c * keys : (c + 2) * keys] = jnp.concatenate(
                [x[:, h * keys : (h + 1) * keys] for x in p[c : c + 2]], axis=1
            )
    lane = lax.broadcasted_iota(jnp.int32, (8, width), 1) // depth
    ones = jnp.ones((value_ref.shape[1], width), jnp.bfloat16)
    for row in range(rows):
        scores = score_ref[row] + bias_ref[...]
        top = jnp.max(scores, axis=1, keepdims=True)
        weights = jnp.exp(scores - top).astype(jnp.bfloat16)
        both = dot(weights, jnp.concatenate([value_ref[row], ones], axis=1))
        for g in range(cols // 8):
            base = g * heads * 8
            pick = both[base : base + 8]
            for h in range(1, heads):
                tile = both[base + h * 8 : base + h * 8 + 8]
                keep = lane == h
                pick = jnp.where(jnp.concatenate([keep, keep], axis=1), tile, pick)
            mixed = pick[:, :width] / pick[:, width:]
            hidden_ref[row * cols + g * 8 : row * cols + g * 8 + 8] = (
                gate_ref[row, g * 8 : g * 8 + 8] * mixed
            )
    result = dot(hidden_ref[...].astype(jnp.bfloat16), wo_ref[...])
    out_ref[...] = result.astype(jnp.bfloat16).reshape(out_ref.shape)


def swap(value, size):
    return lax.ppermute(value, "row", [(i, i ^ 1) for i in range(size)])


def chip_shift(value, size, odd, even):
    pairs = [(i, i ^ (2 * (odd if i % 2 else even))) for i in range(size)]
    return lax.ppermute(value, "row", pairs)


def col_shift(value, row_size, col_size, odd, even):
    pairs = [
        (r * col_size + c, r * col_size + (c ^ (odd if r % 2 else even)))
        for r in range(row_size)
        for c in range(col_size)
    ]
    return lax.ppermute(value, ("row", "col"), pairs)


def pair_up(distances):
    return [tuple(distances[i : i + 2]) for i in range(0, len(distances), 2)]


def row_plan(row_size):
    chips = row_size // 2
    return [chips - 1], pair_up(list(range(1, chips - 1)))


def col_plan(col_size):
    return [1], pair_up(list(reversed(range(2, col_size))))


def per_device(row_size, col_size, pair, group, w_query, w_key, w_value, w_gate, w_bias, w_out):
    heads = w_bias.shape[1]
    rows, cols, _ = group.shape
    width = w_query.shape[1]
    keys = pair.shape[1]
    all_keys = row_size * cols
    shape = jax.ShapeDtypeStruct
    inputs = [pltpu.with_memory_space_constraint(a, pltpu.HBM) for a in (group, pair, w_bias.T)]
    normed, pair, w_bias = call(
        load_kernel,
        (
            shape(group.shape, jnp.bfloat16),
            shape(pair.shape, pair.dtype),
            shape(inputs[2].shape, jnp.float32),
        ),
        inputs,
        10**8,
        [pltpu.VMEM(group.shape, group.dtype), pltpu.SemaphoreType.DMA((3,))],
        pltpu.HBM,
    )
    panel = call(
        bias_kernel, shape((cols * heads // 2, 2 * keys), jnp.float32), [pair, w_bias], 2 * 10**9
    )
    normed = normed[None]
    sibling = swap(normed, row_size)
    stacks, origins = [normed, sibling], [[(0, 0, 0)], [(1, 0, 0)]]
    single, plan = row_plan(row_size)
    for s in single:
        arrived = chip_shift(normed, row_size, s, s)
        stacks += [arrived, swap(arrived, row_size)]
        origins += [[(0, s, s)], [(1, s, s)]]
    both = jnp.concatenate([normed, sibling], axis=0)
    for s, t in plan:
        arrived = chip_shift(both, row_size, s, t)
        stacks += [arrived, swap(arrived, row_size)]
        origins += [[(0, s, t), (1, s, t)], [(1, t, s), (0, t, s)]]
    near, distant = col_plan(col_size)
    panels = [panel]
    for s in near:
        panels.append(col_shift(panel, row_size, col_size, s, s))
    both = jnp.concatenate([panel, swap(panel, row_size)], axis=0)
    for s, t in distant:
        arrived = col_shift(both, row_size, col_size, s, t)
        panels += [arrived, swap(arrived, row_size)]
    keys_shape = shape((rows, all_keys, width), jnp.bfloat16)
    soon = [0, 1] + list(range(2, len(stacks), 2))
    late = list(range(3, len(stacks), 2))
    key, value, gate, queries = call(
        lambda *refs: early_kernel(heads, [origins[i] for i in soon], *refs),
        (
            keys_shape,
            keys_shape,
            shape((rows, cols, width), jnp.float32),
            shape((rows, cols * heads, width), jnp.bfloat16),
        ),
        [stacks[i] for i in soon] + [w_query, w_key, w_value, w_gate],
        10**9,
    )
    late_args = [stacks[i] for i in late] + [queries, w_key, w_value, key, value]
    scores, _, value = call(
        lambda *refs: scores_kernel([origins[i] for i in late], *refs),
        (shape((rows, cols * heads, all_keys), jnp.float32), keys_shape, keys_shape),
        late_args,
        10**9,
        aliases={len(late_args) - 2: 1, len(late_args) - 1: 2},
    )
    return call(
        lambda *refs: attention_kernel(heads, near, distant, *refs),
        shape((rows, cols, w_out.shape[1]), jnp.bfloat16),
        panels + [scores, value, gate, w_out],
        10**9,
        [
            pltpu.VMEM((cols * heads, all_keys), jnp.float32),
            pltpu.VMEM((rows * cols, width), jnp.float32),
        ],
    )


def solution(mesh):
    row_size, col_size = mesh.shape["row"], mesh.shape["col"]
    in_specs = (P("row", "col", None), P("col", "row", None), P(), P(), P(), P(), P(), P())

    def body(*args):
        return per_device(row_size, col_size, *args)

    return jax.shard_map(
        body,
        mesh=mesh,
        in_specs=in_specs,
        out_specs=P("col", "row", None),
        check_vma=False,
    )
```

```python
import math

import jax
import jax.numpy as jnp
from jax import lax
from jax.experimental import pallas as pl
from jax.experimental.pallas import tpu as pltpu
from jax.sharding import PartitionSpec as P


EPS = 1e-05
NT = (((1,), (1,)), ((), ()))
GRANT = 16 << 20
HINT = 10**10
VMEM = pl.BlockSpec(memory_space=pltpu.VMEM)


def call(kernel, outs, args, flops, scratch=(), space=pltpu.VMEM, aliases=None):
    return pl.pallas_call(
        kernel,
        out_shape=outs,
        in_specs=[pl.BlockSpec(memory_space=space)] * len(args),
        out_specs=jax.tree.map(lambda _: VMEM, outs),
        scratch_shapes=list(scratch),
        input_output_aliases=aliases or {},
        cost_estimate=pl.CostEstimate(flops=flops, bytes_accessed=1 << 20, transcendentals=0),
        compiler_params=pltpu.CompilerParams(vmem_limit_bytes=GRANT),
    )(*args)


def dot(a, b):
    return jnp.dot(a, b, preferred_element_type=jnp.float32)


def split(value):
    high = value.astype(jnp.bfloat16)
    return high, value - high.astype(jnp.float32)


def normalize(rows):
    rows = rows.astype(jnp.float32)
    centered = rows - jnp.mean(rows, axis=-1, keepdims=True)
    spread = jnp.mean(centered * centered, axis=-1, keepdims=True)
    return (centered * lax.rsqrt(spread + EPS)).astype(jnp.bfloat16)


def seed_kernel(averages_ref):
    channels = averages_ref.shape[0] // 2
    even = jnp.full((channels, channels), 1.0 / channels, jnp.bfloat16)
    blank = jnp.zeros((channels, channels), jnp.bfloat16)
    averages_ref[...] = jnp.concatenate(
        [jnp.concatenate([even, blank], axis=1), jnp.concatenate([blank, even], axis=1)], axis=0
    )


def front_kernel(group_ref, sibling_ref, pair_ref, w_ref, averages_ref, normed_ref, out_ref):
    normed_ref[0] = normalize(group_ref[0])
    normed_ref[1] = normalize(sibling_ref[0])
    cols, keys, channels = pair_ref.shape
    heads = w_ref.shape[0]
    half = cols // 2
    w = jnp.concatenate([w_ref[...]] * (8 // heads), axis=0)
    w_high, rest = split(w)
    w_mid, rest = split(rest)
    w_sum = jnp.sum(w, axis=1, keepdims=True)
    even = jnp.full((channels, channels), 1.0 / channels, jnp.bfloat16)
    blank = jnp.zeros((channels, channels), jnp.bfloat16)
    pieces = jnp.concatenate([w_high, w_mid, rest.astype(jnp.bfloat16), even[:8]], axis=0)
    left = jnp.concatenate(
        [
            jnp.concatenate([pieces, blank[:96]], axis=0),
            jnp.concatenate([blank[:64], pieces, blank[:32]], axis=0),
        ],
        axis=1,
    )
    tiles = [
        jnp.concatenate([pair_ref[low], pair_ref[low + half]], axis=0) for low in range(half)
    ]
    twins = jnp.concatenate(
        [jnp.concatenate(tiles[low : low + 2], axis=1) for low in range(0, half, 2)], axis=0
    )
    means = dot(twins, averages_ref[...])
    products = lax.dot_general(twins, left, NT, preferred_element_type=jnp.float32)
    height = 2 * keys
    lane = lax.broadcasted_iota(jnp.int32, (height, 128), 1)
    for low in range(0, half, 2):
        rows = slice(low // 2 * height, low // 2 * height + height)
        centered = twins[rows].astype(jnp.float32) - means[rows]
        squares = centered * centered
        first = jnp.sum(squares[:, :channels], axis=1, keepdims=True)
        second = jnp.sum(squares[:, channels:], axis=1, keepdims=True)
        mixed = jnp.where(
            (lane & 32) == 0, products[rows], jnp.where(lane < 64, first, second)
        ).T
        for twin in range(2):
            t = mixed[twin * 64 : twin * 64 + 64]
            total = t[0:8] + t[8:16] + t[16:24] - t[24:32] * w_sum
            bias = total * lax.rsqrt(t[32:40] * (1.0 / channels) + EPS)
            at = low + twin
            out_ref[pl.ds((at // 8) * 8 * heads + at % 8, heads, stride=8), :] = bias[0:heads]


def place_blocks(sources, origins, w_value, rows_ref, value_ref):
    _, rows, cols, channels = sources[0].shape
    me = lax.axis_index("row")
    for ref, entry, (flip, odd, even, raw) in [
        (ref, entry, origin)
        for ref, group in zip(sources, origins)
        for entry, origin in enumerate(group)
    ]:
        block = normalize(ref[entry]) if raw else ref[entry]
        core = me & 1
        chip = (me >> 1) ^ jnp.where(core == 1, odd, even)
        place = pl.ds(pl.multiple_of((2 * chip + (core ^ flip)) * cols, cols), cols)
        rows_ref[:, place, :] = block
        value = dot(block.reshape(rows * cols, channels), w_value).astype(jnp.bfloat16)
        value_ref[:, place, :] = value.reshape(rows, cols, value.shape[1])


def early_kernel(heads, origins, *refs):
    sources = refs[: len(origins)]
    wq_ref, wk_ref, wv_ref, wg_ref, rows_ref, value_ref, gate_ref, stack_ref = refs[len(origins) :]
    _, rows, cols, channels = sources[0].shape
    width = wq_ref.shape[1]
    depth = width // heads
    own = sources[0][0].reshape(rows * cols, channels)
    both = dot(own, jnp.concatenate([wq_ref[...], wg_ref[...]], axis=1))
    gate_ref[...] = jax.nn.sigmoid(both[:, width:]).reshape(rows, cols, width)
    query = both[:, :width] * (1.0 / math.sqrt(depth))
    lane = lax.broadcasted_iota(jnp.int32, (8, width), 1) // depth
    for row in range(rows):
        tiles = []
        for g in range(cols // 8):
            tile = query[row * cols + g * 8 : row * cols + g * 8 + 8]
            for h in range(heads):
                tiles.append(jnp.where(lane == h, tile, 0.0))
        stacked = jnp.concatenate(tiles, axis=0).astype(jnp.bfloat16)
        stack_ref[row] = lax.dot_general(
            stacked, wk_ref[...], NT, preferred_element_type=jnp.float32
        ).astype(jnp.bfloat16)
    place_blocks(sources, origins, wv_ref[...], rows_ref, value_ref)


def scores_kernel(origins, *refs):
    sources = refs[: len(origins)]
    stack_ref, wv_ref, _, _, score_ref, rows_ref, value_ref = refs[len(origins) :]
    place_blocks(sources, origins, wv_ref[...], rows_ref, value_ref)
    for row in range(stack_ref.shape[0]):
        score_ref[row] = lax.dot_general(
            stack_ref[row], rows_ref[row], NT, preferred_element_type=jnp.float32
        )


def attention_kernel(heads, single, plan, *refs):
    sources = 1 + len(single) + 2 * len(plan)
    score_ref, value_ref, gate_ref, wo_ref, out_ref, bias_ref, hidden_ref = refs[sources:]
    rows, cols, width = gate_ref.shape
    depth = width // heads
    half, keys = refs[0].shape[0], refs[0].shape[1] // 2
    odd = (lax.axis_index("row") & 1) == 1
    me = lax.axis_index("col")
    parts = sources
    p = [refs[0][...]] + [None] * (parts - 1)
    for at, s in enumerate(single):
        p[s] = refs[1 + at][...]
    for at, (s, t) in enumerate(plan):
        arrived = refs[1 + len(single) + 2 * at][:half]
        passed = refs[2 + len(single) + 2 * at][half:]
        p[s] = jnp.where(odd, arrived, passed)
        p[t] = jnp.where(odd, passed, arrived)
    bit = 1
    while bit < parts:
        turn = (me & bit) != 0
        p = [jnp.where(turn, p[k ^ bit], p[k]) for k in range(parts)]
        bit *= 2
    for h in range(2):
        for c in range(0, parts, 2):
            bias_ref[h * half : (h + 1) * half, c * keys : (c + 2) * keys] = jnp.concatenate(
                [x[:, h * keys : (h + 1) * keys] for x in p[c : c + 2]], axis=1
            )
    lane = lax.broadcasted_iota(jnp.int32, (8, width), 1) // depth
    ones = jnp.ones((value_ref.shape[1], width), jnp.bfloat16)
    for row in range(rows):
        scores = score_ref[row] + bias_ref[...]
        top = jnp.max(scores, axis=1, keepdims=True)
        weights = jnp.exp(scores - top).astype(jnp.bfloat16)
        both = dot(weights, jnp.concatenate([value_ref[row], ones], axis=1))
        for g in range(cols // 8):
            base = g * heads * 8
            pick = both[base : base + 8]
            for h in range(1, heads):
                tile = both[base + h * 8 : base + h * 8 + 8]
                keep = lane == h
                pick = jnp.where(jnp.concatenate([keep, keep], axis=1), tile, pick)
            mixed = pick[:, :width] / pick[:, width:]
            hidden_ref[row * cols + g * 8 : row * cols + g * 8 + 8] = (
                gate_ref[row, g * 8 : g * 8 + 8] * mixed
            )
    result = dot(hidden_ref[...].astype(jnp.bfloat16), wo_ref[...])
    out_ref[...] = result.astype(jnp.bfloat16).reshape(out_ref.shape)


def swap(value, size):
    return lax.ppermute(value, "row", [(i, i ^ 1) for i in range(size)])


def chip_shift(value, size, odd, even):
    pairs = [(i, i ^ (2 * (odd if i % 2 else even))) for i in range(size)]
    return lax.ppermute(value, "row", pairs)


def col_shift(value, row_size, col_size, odd, even):
    pairs = [
        (r * col_size + c, r * col_size + (c ^ (odd if r % 2 else even)))
        for r in range(row_size)
        for c in range(col_size)
    ]
    return lax.ppermute(value, ("row", "col"), pairs)


def pair_up(distances):
    return [tuple(distances[i : i + 2]) for i in range(0, len(distances), 2)]


def row_plan(row_size):
    chips = row_size // 2
    return [chips - 1], pair_up(list(range(1, chips - 1)))


def col_plan(col_size):
    distances = list(reversed(range(1, col_size)))
    middle = col_size // 2
    distances.remove(middle)
    return [middle], pair_up(distances)


def per_device(row_size, col_size, pair, group, w_query, w_key, w_value, w_gate, w_bias, w_out):
    heads = w_bias.shape[1]
    rows, cols, channels = group.shape
    width = w_query.shape[1]
    keys = pair.shape[1]
    all_keys = row_size * cols
    shape = jax.ShapeDtypeStruct
    averages = call(seed_kernel, shape((2 * channels, 2 * channels), jnp.bfloat16), [], HINT)
    single, plan = row_plan(row_size)
    raw = group[None]
    sibling = swap(raw, row_size)
    early, late = [], []
    for s in single:
        arrived = chip_shift(raw, row_size, s, s)
        early.append((arrived, [(0, s, s, True)]))
        late.append((swap(arrived, row_size), [(1, s, s, True)]))
    both, panel = call(
        front_kernel,
        (
            shape((2,) + group.shape, jnp.bfloat16),
            shape((cols * heads // 2, 2 * keys), jnp.float32),
        ),
        [raw, sibling, pair, w_bias.T, averages],
        2 * 10**9,
    )
    early.insert(0, (both, [(0, 0, 0, False), (1, 0, 0, False)]))
    for s, t in plan:
        arrived = chip_shift(both, row_size, s, t)
        early.append((arrived, [(0, s, t, False), (1, s, t, False)]))
        passed = swap(arrived, row_size)
        late.append((passed, [(1, t, s, False), (0, t, s, False)]))
    near, distant = col_plan(col_size)
    panels = [panel]
    for s in near:
        panels.append(col_shift(panel, row_size, col_size, s, s))
    both = jnp.concatenate([panel, swap(panel, row_size)], axis=0)
    for s, t in distant:
        arrived = col_shift(both, row_size, col_size, s, t)
        panels += [arrived, swap(arrived, row_size)]
    keys_shape = shape((rows, all_keys, channels), jnp.bfloat16)
    value_shape = shape((rows, all_keys, width), jnp.bfloat16)
    normed, value, gate, queries = call(
        lambda *refs: early_kernel(heads, [origin for _, origin in early], *refs),
        (
            keys_shape,
            value_shape,
            shape((rows, cols, width), jnp.float32),
            shape((rows, cols * heads, channels), jnp.bfloat16),
        ),
        [block for block, _ in early] + [w_query, w_key, w_value, w_gate],
        10**9,
    )
    late_args = [block for block, _ in late] + [queries, w_value, normed, value]
    scores, _, value = call(
        lambda *refs: scores_kernel([origin for _, origin in late], *refs),
        (shape((rows, cols * heads, all_keys), jnp.float32), keys_shape, value_shape),
        late_args,
        10**9,
        aliases={len(late_args) - 2: 1, len(late_args) - 1: 2},
    )
    return call(
        lambda *refs: attention_kernel(heads, near, distant, *refs),
        shape((rows, cols, w_out.shape[1]), jnp.bfloat16),
        panels + [scores, value, gate, w_out],
        10**9,
        [
            pltpu.VMEM((cols * heads, all_keys), jnp.float32),
            pltpu.VMEM((rows * cols, width), jnp.float32),
        ],
    )


def solution(mesh):
    row_size, col_size = mesh.shape["row"], mesh.shape["col"]
    in_specs = (P("row", "col", None), P("col", "row", None), P(), P(), P(), P(), P(), P())

    def body(*args):
        return per_device(row_size, col_size, *args)

    return jax.shard_map(
        body,
        mesh=mesh,
        in_specs=in_specs,
        out_specs=P("col", "row", None),
        check_vma=False,
    )
```

```python
import math

import jax
import jax.numpy as jnp
from jax import lax
from jax.experimental import pallas as pl
from jax.experimental.pallas import tpu as pltpu
from jax.sharding import PartitionSpec as P


EPS = 1e-05
NT = (((1,), (1,)), ((), ()))
GRANT = 16 << 20
HINT = 10**10
LOG2E = math.log2(math.e)
VMEM = pl.BlockSpec(memory_space=pltpu.VMEM)


def call(kernel, outs, args, flops, scratch=(), space=pltpu.VMEM, aliases=None):
    return pl.pallas_call(
        kernel,
        out_shape=outs,
        in_specs=[pl.BlockSpec(memory_space=space)] * len(args),
        out_specs=jax.tree.map(lambda _: VMEM, outs),
        scratch_shapes=list(scratch),
        input_output_aliases=aliases or {},
        cost_estimate=pl.CostEstimate(flops=flops, bytes_accessed=1 << 20, transcendentals=0),
        compiler_params=pltpu.CompilerParams(vmem_limit_bytes=GRANT),
    )(*args)


def dot(a, b):
    return jnp.dot(a, b, preferred_element_type=jnp.float32)


def split(value):
    high = value.astype(jnp.bfloat16)
    return high, value - high.astype(jnp.float32)


def normalize(rows):
    rows = rows.astype(jnp.float32)
    centered = rows - jnp.mean(rows, axis=-1, keepdims=True)
    spread = jnp.mean(centered * centered, axis=-1, keepdims=True)
    return (centered * lax.rsqrt(spread + EPS)).astype(jnp.bfloat16)


def seed_kernel(averages_ref):
    channels = averages_ref.shape[0] // 2
    even = jnp.full((channels, channels), 1.0 / channels, jnp.bfloat16)
    blank = jnp.zeros((channels, channels), jnp.bfloat16)
    averages_ref[...] = jnp.concatenate(
        [jnp.concatenate([even, blank], axis=1), jnp.concatenate([blank, even], axis=1)], axis=0
    )


def front_kernel(group_ref, sibling_ref, pair_ref, w_ref, averages_ref, normed_ref, out_ref):
    normed_ref[0] = normalize(group_ref[0])
    normed_ref[1] = normalize(sibling_ref[0])
    cols, keys, channels = pair_ref.shape
    heads = w_ref.shape[0]
    half = cols // 2
    w = jnp.concatenate([w_ref[...]] * (8 // heads), axis=0)
    w_high, rest = split(w)
    w_mid, rest = split(rest)
    w_sum = jnp.sum(w, axis=1, keepdims=True)
    even = jnp.full((channels, channels), 1.0 / channels, jnp.bfloat16)
    blank = jnp.zeros((channels, channels), jnp.bfloat16)
    pieces = jnp.concatenate([w_high, w_mid, rest.astype(jnp.bfloat16), even[:8]], axis=0)
    left = jnp.concatenate(
        [
            jnp.concatenate([pieces, blank[:96]], axis=0),
            jnp.concatenate([blank[:64], pieces, blank[:32]], axis=0),
        ],
        axis=1,
    )
    tiles = [
        jnp.concatenate([pair_ref[low], pair_ref[low + half]], axis=0) for low in range(half)
    ]
    twins = jnp.concatenate(
        [jnp.concatenate(tiles[low : low + 2], axis=1) for low in range(0, half, 2)], axis=0
    )
    means = dot(twins, averages_ref[...])
    products = lax.dot_general(twins, left, NT, preferred_element_type=jnp.float32)
    height = 2 * keys
    lane = lax.broadcasted_iota(jnp.int32, (height, 128), 1)
    for low in range(0, half, 2):
        rows = slice(low // 2 * height, low // 2 * height + height)
        centered = twins[rows].astype(jnp.float32) - means[rows]
        squares = centered * centered
        first = jnp.sum(squares[:, :channels], axis=1, keepdims=True)
        second = jnp.sum(squares[:, channels:], axis=1, keepdims=True)
        mixed = jnp.where(
            (lane & 32) == 0, products[rows], jnp.where(lane < 64, first, second)
        ).T
        for twin in range(2):
            t = mixed[twin * 64 : twin * 64 + 64]
            total = t[0:8] + t[8:16] + t[16:24] - t[24:32] * w_sum
            bias = total * (lax.rsqrt(t[32:40] * (1.0 / channels) + EPS) * LOG2E)
            at = low + twin
            out_ref[pl.ds((at // 8) * 8 * heads + at % 8, heads, stride=8), :] = bias[0:heads]


def place_blocks(sources, origins, w_value, rows_ref, value_ref):
    _, rows, cols, channels = sources[0].shape
    me = lax.axis_index("row")
    for ref, entry, (flip, odd, even, raw) in [
        (ref, entry, origin)
        for ref, group in zip(sources, origins)
        for entry, origin in enumerate(group)
    ]:
        block = normalize(ref[entry]) if raw else ref[entry]
        core = me & 1
        chip = (me >> 1) ^ jnp.where(core == 1, odd, even)
        place = pl.ds(pl.multiple_of((2 * chip + (core ^ flip)) * cols, cols), cols)
        rows_ref[:, place, :] = block
        value = dot(block.reshape(rows * cols, channels), w_value).astype(jnp.bfloat16)
        value_ref[:, place, :] = value.reshape(rows, cols, value.shape[1])


def early_kernel(heads, origins, *refs):
    sources = refs[: len(origins)]
    wq_ref, wk_ref, wv_ref, wg_ref, rows_ref, value_ref, gate_ref, stack_ref = refs[len(origins) :]
    _, rows, cols, channels = sources[0].shape
    width = wq_ref.shape[1]
    depth = width // heads
    own = sources[0][0].reshape(rows * cols, channels)
    both = dot(own, jnp.concatenate([wq_ref[...], wg_ref[...]], axis=1))
    gate_ref[...] = jax.nn.sigmoid(both[:, width:]).reshape(rows, cols, width)
    query = both[:, :width] * (1.0 / math.sqrt(depth))
    lane = lax.broadcasted_iota(jnp.int32, (8, width), 1) // depth
    for row in range(rows):
        tiles = []
        for g in range(cols // 8):
            tile = query[row * cols + g * 8 : row * cols + g * 8 + 8]
            for h in range(heads):
                tiles.append(jnp.where(lane == h, tile, 0.0))
        stacked = jnp.concatenate(tiles, axis=0).astype(jnp.bfloat16)
        turned = lax.dot_general(
            stacked, wk_ref[...], NT, preferred_element_type=jnp.float32
        )
        stack_ref[row] = (turned * LOG2E).astype(jnp.bfloat16)
    place_blocks(sources, origins, wv_ref[...], rows_ref, value_ref)


def scores_kernel(origins, *refs):
    sources = refs[: len(origins)]
    stack_ref, wv_ref, _, _, score_ref, rows_ref, value_ref = refs[len(origins) :]
    place_blocks(sources, origins, wv_ref[...], rows_ref, value_ref)
    for row in range(stack_ref.shape[0]):
        score_ref[row] = lax.dot_general(
            stack_ref[row], rows_ref[row], NT, preferred_element_type=jnp.float32
        )


def attention_kernel(heads, single, plan, *refs):
    sources = 1 + len(single) + 2 * len(plan)
    score_ref, value_ref, gate_ref, wo_ref, out_ref, bias_ref, hidden_ref = refs[sources:]
    rows, cols, width = gate_ref.shape
    depth = width // heads
    half, keys = refs[0].shape[0], refs[0].shape[1] // 2
    odd = (lax.axis_index("row") & 1) == 1
    me = lax.axis_index("col")
    parts = sources
    p = [refs[0][...]] + [None] * (parts - 1)
    for at, s in enumerate(single):
        p[s] = refs[1 + at][...]
    for at, (s, t) in enumerate(plan):
        arrived = refs[1 + len(single) + 2 * at][:half]
        passed = refs[2 + len(single) + 2 * at][half:]
        p[s] = jnp.where(odd, arrived, passed)
        p[t] = jnp.where(odd, passed, arrived)
    bit = 1
    while bit < parts:
        turn = (me & bit) != 0
        p = [jnp.where(turn, p[k ^ bit], p[k]) for k in range(parts)]
        bit *= 2
    for h in range(2):
        for c in range(0, parts, 2):
            bias_ref[h * half : (h + 1) * half, c * keys : (c + 2) * keys] = jnp.concatenate(
                [x[:, h * keys : (h + 1) * keys] for x in p[c : c + 2]], axis=1
            )
    lane = lax.broadcasted_iota(jnp.int32, (8, width), 1) // depth
    ones = jnp.ones((value_ref.shape[1], width), jnp.bfloat16)
    for row in range(rows):
        scores = score_ref[row] + bias_ref[...]
        top = jnp.max(scores, axis=1, keepdims=True)
        weights = jnp.exp2(scores - top).astype(jnp.bfloat16)
        both = dot(weights, jnp.concatenate([value_ref[row], ones], axis=1))
        for g in range(cols // 8):
            base = g * heads * 8
            pick = both[base : base + 8]
            for h in range(1, heads):
                tile = both[base + h * 8 : base + h * 8 + 8]
                keep = lane == h
                pick = jnp.where(jnp.concatenate([keep, keep], axis=1), tile, pick)
            mixed = pick[:, :width] / pick[:, width:]
            hidden_ref[row * cols + g * 8 : row * cols + g * 8 + 8] = (
                gate_ref[row, g * 8 : g * 8 + 8] * mixed
            )
    result = dot(hidden_ref[...].astype(jnp.bfloat16), wo_ref[...])
    out_ref[...] = result.astype(jnp.bfloat16).reshape(out_ref.shape)


def swap(value, size):
    return lax.ppermute(value, "row", [(i, i ^ 1) for i in range(size)])


def chip_shift(value, size, odd, even):
    pairs = [(i, i ^ (2 * (odd if i % 2 else even))) for i in range(size)]
    return lax.ppermute(value, "row", pairs)


def col_shift(value, row_size, col_size, odd, even):
    pairs = [
        (r * col_size + c, r * col_size + (c ^ (odd if r % 2 else even)))
        for r in range(row_size)
        for c in range(col_size)
    ]
    return lax.ppermute(value, ("row", "col"), pairs)


def pair_up(distances):
    return [tuple(distances[i : i + 2]) for i in range(0, len(distances), 2)]


def row_plan(row_size):
    chips = row_size // 2
    return [chips - 1], pair_up(list(range(1, chips - 1)))


def col_plan(col_size):
    distances = list(reversed(range(1, col_size)))
    middle = col_size // 2
    distances.remove(middle)
    return [middle], pair_up(distances)


def per_device(row_size, col_size, pair, group, w_query, w_key, w_value, w_gate, w_bias, w_out):
    heads = w_bias.shape[1]
    rows, cols, channels = group.shape
    width = w_query.shape[1]
    keys = pair.shape[1]
    all_keys = row_size * cols
    shape = jax.ShapeDtypeStruct
    averages = call(seed_kernel, shape((2 * channels, 2 * channels), jnp.bfloat16), [], HINT)
    single, plan = row_plan(row_size)
    raw = group[None]
    sibling = swap(raw, row_size)
    early, late = [], []
    for s in single:
        arrived = chip_shift(raw, row_size, s, s)
        early.append((arrived, [(0, s, s, True)]))
        late.append((swap(arrived, row_size), [(1, s, s, True)]))
    both, panel = call(
        front_kernel,
        (
            shape((2,) + group.shape, jnp.bfloat16),
            shape((cols * heads // 2, 2 * keys), jnp.float32),
        ),
        [raw, sibling, pair, w_bias.T, averages],
        2 * 10**9,
    )
    early.insert(0, (both, [(0, 0, 0, False), (1, 0, 0, False)]))
    for s, t in plan:
        arrived = chip_shift(both, row_size, s, t)
        early.append((arrived, [(0, s, t, False), (1, s, t, False)]))
        passed = swap(arrived, row_size)
        late.append((passed, [(1, t, s, False), (0, t, s, False)]))
    near, distant = col_plan(col_size)
    panels = [panel]
    for s in near:
        panels.append(col_shift(panel, row_size, col_size, s, s))
    both = jnp.concatenate([panel, swap(panel, row_size)], axis=0)
    for s, t in distant:
        arrived = col_shift(both, row_size, col_size, s, t)
        panels += [arrived, swap(arrived, row_size)]
    keys_shape = shape((rows, all_keys, channels), jnp.bfloat16)
    value_shape = shape((rows, all_keys, width), jnp.bfloat16)
    normed, value, gate, queries = call(
        lambda *refs: early_kernel(heads, [origin for _, origin in early], *refs),
        (
            keys_shape,
            value_shape,
            shape((rows, cols, width), jnp.float32),
            shape((rows, cols * heads, channels), jnp.bfloat16),
        ),
        [block for block, _ in early] + [w_query, w_key, w_value, w_gate],
        10**9,
    )
    late_args = [block for block, _ in late] + [queries, w_value, normed, value]
    scores, _, value = call(
        lambda *refs: scores_kernel([origin for _, origin in late], *refs),
        (shape((rows, cols * heads, all_keys), jnp.float32), keys_shape, value_shape),
        late_args,
        10**9,
        aliases={len(late_args) - 2: 1, len(late_args) - 1: 2},
    )
    return call(
        lambda *refs: attention_kernel(heads, near, distant, *refs),
        shape((rows, cols, w_out.shape[1]), jnp.bfloat16),
        panels + [scores, value, gate, w_out],
        10**9,
        [
            pltpu.VMEM((cols * heads, all_keys), jnp.float32),
            pltpu.VMEM((rows * cols, width), jnp.float32),
        ],
    )


def solution(mesh):
    row_size, col_size = mesh.shape["row"], mesh.shape["col"]
    in_specs = (P("row", "col", None), P("col", "row", None), P(), P(), P(), P(), P(), P())

    def body(*args):
        return per_device(row_size, col_size, *args)

    return jax.shard_map(
        body,
        mesh=mesh,
        in_specs=in_specs,
        out_specs=P("col", "row", None),
        check_vma=False,
    )
```
